32 devices in a mesh: row: 4 (over y, x), col: 4 (over z), rep: 2 (over core).
Axes of the slice: x: 2, y: 2, z: 4, core: 2. Of those that a mesh axis runs over, the one named last changes fastest.
Arguments:
- sources: int32 [64], replicated, may hold values from 0 to 4095
- tile_weights: int32 [1024, 128, 128], P(('row', 'col', 'rep')), may hold values from 0 to 16, as said below
- tile_src: int32 [1024], P(('row', 'col', 'rep')), may hold values from 0 to 31, as said below
- tile_dst: int32 [1024], P(('row', 'col', 'rep')), may hold values from 0 to 31, as said below
- tile_count: int32 [32], P(('row', 'col', 'rep')), may hold values from 1 to 32, 512 in all
Outputs:
- distances: float32 [64, 4096], P(None, ('row', 'col', 'rep'))
- recip_sums: float32 [16, 64], P(('row', 'col'))
The draws below stay inside these ranges and needn't reach their ends.
Inputs may be any that keep to these rules, and one draw needn't show every extreme that they name: `tile_weights`: an entry of 0 means no edge; others are the edge's weight. `tile_src`: piece p = b // 1 of block b belongs to the device at mesh coordinates (row, col, rep) = (p // 8, (p // 2) % 4, p % 2); slot k belongs to device k // 32 in the same numbering. A tile's source block lies in a piece whose col index is that of the tile's device. `tile_dst`: A tile's destination block lies in a piece whose row and rep indices are those of the tile's device, in the numbering given for tile_src. Only the first tile_count[d] slots of device d hold live tiles; some device has all 32 slots live.
All inputs are finite; a program needn't handle non-finite values.
Results may differ from the reference program's by a relative error of at most 0.0003.
Values may be sent and summed in bfloat16 or wider, within the bound.
No kernel may reach another device: no remote copies, remote signals or barrier semaphores. Data moves between devices by JAX's collectives and lax.ppermute only.
A program may use at most 64 MiB of HBM per device.

```python
import math
import jax
import jax.numpy as jnp
import numpy as np
from jax import lax

SOURCES = 64
BLK_DEV = 1
TILE_DEV = 32
BS = 128
ROUNDS = 2
SECTIONS = 4
OWNERS = 4
HALVES = 2
VERTS = 4096
NTILES = 1024
DEVICES = 32


def tile_place(key, which):
    slot_ids = jnp.arange(NTILES, dtype=jnp.int32)
    device = slot_ids // TILE_DEV
    section = device // (OWNERS * HALVES)
    owner = device // HALVES % OWNERS
    half_id = device % HALVES
    folded = jax.random.fold_in(key, which)
    key_one, key_two, key_three = jax.random.split(folded, 3)
    block_in = jax.random.randint(key_three, (NTILES,), 0, BLK_DEV, dtype=jnp.int32)
    if which == 11:
        other_sec = jax.random.randint(key_one, (NTILES,), 0, SECTIONS, dtype=jnp.int32)
        other_half = jax.random.randint(key_two, (NTILES,), 0, HALVES, dtype=jnp.int32)
        piece_id = (other_sec * OWNERS + owner) * HALVES + other_half
    else:
        other_owner = jax.random.randint(key_one, (NTILES,), 0, OWNERS, dtype=jnp.int32)
        piece_id = (section * OWNERS + other_owner) * HALVES + half_id
    return (piece_id * BLK_DEV + block_in).astype(jnp.int32)


def draw_tile_src(key, part):
    return tile_place(key, 11)


def draw_tile_dst(key, part):
    return tile_place(key, 12)


def draw_tile_weights(key, part):
    folded = jax.random.fold_in(key, 13)
    key_one, key_two = jax.random.split(folded)
    is_edge = jax.random.randint(key_one, (NTILES, BS, BS), 0, 5, dtype=jnp.int32) == 0
    weight = jax.random.randint(key_two, (NTILES, BS, BS), 1, 17, dtype=jnp.int32)
    return jnp.where(is_edge, weight, 0).astype(jnp.int32)


def set_ends(result, key, least, top_value):
    index_at = [jax.random.randint(jax.random.fold_in(key, axis), (), 0, length) for axis, length in enumerate(result.shape)]
    longest = result.shape.index(max(result.shape))
    neighbour = index_at[:longest] + [(index_at[longest] + 1) % result.shape[longest]] + index_at[longest + 1:]
    return result.at[tuple(index_at)].set(least).at[tuple(neighbour)].set(top_value)


def split_up(amount, total, most, slope):
    loads = [(1 << 20) // math.isqrt(grade ** slope) + 1 for grade in range(2, amount + 1)]
    rest, holding = total - most - (amount - 1), [1] * (amount - 1)
    while rest > 0:
        movable = [i for i in range(amount - 1) if holding[i] < most]
        pool, budget = sum([loads[i] for i in movable]), rest
        for i in movable:
            addition = min(most - holding[i], max(1, budget * loads[i] // pool), rest)
            holding[i] = holding[i] + addition
            rest = rest - addition
    return np.array([most] + holding)


def ragged_sizes(stream_key, amount, total, limit, lean):
    if amount == 2:
        one = jax.random.randint(stream_key, (), max(1, total - limit), min(limit, total - 1) + 1)
        return jnp.stack([one, total - one])
    lengths = jnp.asarray(split_up(amount, total, limit, lean), jnp.int32)
    couples = (amount - 1) // 2
    donor, taker = lengths[1:1 + 2 * couples:2], lengths[2:2 + 2 * couples:2]
    margin = jnp.minimum(donor - 1, limit - taker)
    moved = jax.random.randint(jax.random.fold_in(stream_key, 1), (couples,), 0, 1 << 20) % (margin + 1)
    lengths = lengths.at[1:1 + 2 * couples:2].set(donor - moved).at[2:2 + 2 * couples:2].set(taker + moved)
    return lengths[jax.random.permutation(jax.random.fold_in(stream_key, 2), amount)]


def setup_inputs(seed: int = 0) -> dict:
    key_of = jax.random.split(jax.random.key(seed), 6)
    return {
        "sources": set_ends(jax.random.randint(key_of[0], (SOURCES,), 0, VERTS), jax.random.fold_in(key_of[0], 1), 0, VERTS - 1).astype(jnp.int32),
        "tile_weights": draw_tile_weights(jax.random.fold_in(key_of[5], 71), 0),
        "tile_src": draw_tile_src(jax.random.fold_in(key_of[5], 71), 0),
        "tile_dst": draw_tile_dst(jax.random.fold_in(key_of[5], 71), 0),
        "tile_count": ragged_sizes(key_of[4], DEVICES, DEVICES * TILE_DEV // 2, TILE_DEV, 2).astype(jnp.int32),
    }


far_value = 255.0


def reference(sources, tile_weights, tile_src, tile_dst, tile_count):
    blocks = VERTS // BS
    slot_ids = jnp.arange(NTILES, dtype=jnp.int32)
    live_slots = (slot_ids % TILE_DEV) < tile_count[slot_ids // TILE_DEV]
    weights = jnp.where(tile_weights > 0, tile_weights.astype(jnp.float32), far_value)
    columns = jnp.arange(VERTS, dtype=jnp.int32)
    dist = jnp.where(columns[None, :] == sources[:, None], 0.0, far_value).astype(jnp.bfloat16)
    packed = (tile_src.reshape(DEVICES, TILE_DEV), tile_dst.reshape(DEVICES, TILE_DEV),
              weights.reshape(DEVICES, TILE_DEV, BS, BS), live_slots.reshape(DEVICES, TILE_DEV))
    for round_no in range(ROUNDS):
        blocked = dist.astype(jnp.float32).reshape(SOURCES, blocks, BS).transpose(1, 0, 2)

        def relax(best_seen, device_group):
            src_ids, dst_ids, weight_rows, live_rows = device_group
            source_rows = blocked[src_ids]
            candidate = jnp.min(source_rows[:, :, :, None] + weight_rows[:, None, :, :], axis=2)
            candidate = jnp.where(live_rows[:, None, None], candidate, far_value)
            return best_seen.at[dst_ids].min(candidate), None

        start_best = jnp.full((blocks, SOURCES, BS), far_value, jnp.float32)
        best_seen, _ = lax.scan(relax, start_best, packed)
        fresh = best_seen.transpose(1, 0, 2).reshape(SOURCES, VERTS)
        dist = jnp.minimum(dist, fresh.astype(jnp.bfloat16))
    as_float = dist.astype(jnp.float32)
    inverse = jnp.where(as_float > 0, 1.0 / jnp.maximum(as_float, 1.0), 0.0)
    chip_sums = jnp.sum(inverse.reshape(SOURCES, SECTIONS * OWNERS, HALVES * BLK_DEV * BS), axis=2)
    return as_float, chip_sums.transpose(1, 0)
```

```python
import functools

import jax
import jax.numpy as jnp
from jax import lax
from jax.experimental import pallas as pl
from jax.experimental.pallas import tpu as pltpu
from jax.sharding import PartitionSpec as P

BLK_DEV = 1
STEP = 7.5
HALF = 63.0
FAR = 255.0
CHUNKS = 4


def first_kernel(n_row, n_col, n_rep, src, dst, count, sources, weights, code, part, hot, best, raw, sems):
    tiles, size, _ = code.shape
    height = hot.shape[1]
    step = tiles // CHUNKS
    copies = [
        pltpu.make_async_copy(
            weights.at[pl.ds(c * step, step)], raw.at[pl.ds(c * step, step)], sems.at[c]
        )
        for c in range(CHUNKS)
    ]
    for copy in copies:
        copy.start()
    col = lax.axis_index("col")
    wanted = jnp.broadcast_to(sources[...], (size, height)).T
    lane = lax.broadcasted_iota(jnp.int32, (height, size), 1)
    for q in range(n_row * n_rep):
        block = ((q // n_rep) * n_col + col) * n_rep + q % n_rep
        hot[q] = jnp.where(wanted == lane + block * size, 2.0**HALF, 0.0).astype(jnp.bfloat16)
    best[...] = jnp.zeros_like(best)
    live = count[0]
    for c, copy in enumerate(copies):
        copy.wait()
        for k in range(c * step, (c + 1) * step):
            w = raw[k].astype(jnp.float32)
            bound = jnp.where(k < live, 0.5, 1e9)
            coded = jnp.where(w > bound, jnp.exp2(HALF - STEP * w), 0.0).astype(jnp.bfloat16)
            code[k] = coded
            piece = src[k] // BLK_DEV
            q = piece // (n_col * n_rep) * n_rep + lax.rem(piece, n_rep)
            total = jnp.dot(hot[q], coded, preferred_element_type=jnp.float32)
            d = lax.rem(dst[k] // BLK_DEV // n_rep, n_col)
            best[d] = jnp.maximum(best[d], total)
    part[...] = (best[...] * 2.0**-HALF).astype(jnp.bfloat16)


def second_kernel(n_row, n_col, n_rep, src, dst, dist, code, part, best):
    best[...] = jnp.zeros_like(best)
    for k in range(code.shape[0]):
        piece = src[k] // BLK_DEV
        q = piece // (n_col * n_rep) * n_rep + lax.rem(piece, n_rep)
        total = jnp.dot(dist[q], code[k], preferred_element_type=jnp.float32)
        d = lax.rem(dst[k] // BLK_DEV // n_rep, n_col)
        best[d] = jnp.maximum(best[d], total)
    part[...] = best[...].astype(jnp.bfloat16)


def final_kernel(fresh, own, distances, sums):
    best = jnp.max(fresh[...].astype(jnp.float32), axis=0)
    best = jnp.maximum(best, own[...].astype(jnp.float32) * 2.0**HALF)
    level = jnp.ceil((2 * HALF - 0.22 - jnp.log2(jnp.maximum(best, 2.0**-125))) / STEP)
    value = jnp.where(best > 0.0, level, FAR)
    distances[...] = value
    inverse = jnp.where(value > 0.0, 1.0 / jnp.maximum(value, 1.0), 0.0)
    sums[...] = jnp.sum(inverse.T, axis=0, keepdims=True)


def per_device(sources, tile_weights, tile_src, tile_dst, tile_count):
    n_row, n_col, n_rep = (lax.axis_size(a) for a in ("row", "col", "rep"))
    height = sources.shape[0]
    tiles, size, _ = tile_weights.shape
    smem = pl.BlockSpec(memory_space=pltpu.SMEM)
    vmem = pl.BlockSpec(memory_space=pltpu.VMEM)
    sizes = (n_row, n_col, n_rep)
    code, part = pl.pallas_call(
        functools.partial(first_kernel, *sizes),
        out_shape=(
            jax.ShapeDtypeStruct((tiles, size, size), jnp.bfloat16),
            jax.ShapeDtypeStruct((n_col, height, size), jnp.bfloat16),
        ),
        in_specs=[smem, smem, smem, vmem, pl.BlockSpec(memory_space=pl.ANY)],
        out_specs=(vmem, vmem),
        scratch_shapes=[
            pltpu.VMEM((n_row * n_rep, height, size), jnp.bfloat16),
            pltpu.VMEM((n_col, height, size), jnp.float32),
            pltpu.VMEM((tiles, size, size), jnp.int32),
            pltpu.SemaphoreType.DMA((CHUNKS,)),
        ],
        name="round_one",
    )(tile_src, tile_dst, tile_count, sources.reshape(1, height), tile_weights)
    piece = (lax.axis_index("row") * n_col + lax.axis_index("col")) * n_rep + lax.axis_index("rep")
    columns = piece * size + jnp.arange(size, dtype=jnp.int32)
    start = jnp.where(columns[None, :] == sources[:, None], 2.0**HALF, 0.0).astype(jnp.bfloat16)
    fresh = lax.all_to_all(part, "col", 0, 0)
    own = jnp.maximum(jnp.max(fresh, axis=0), start)
    dist = lax.all_gather(own, ("row", "rep"), axis=0)
    part = pl.pallas_call(
        functools.partial(second_kernel, *sizes),
        out_shape=jax.ShapeDtypeStruct((n_col, height, size), jnp.bfloat16),
        in_specs=[smem, smem, vmem, vmem],
        out_specs=vmem,
        scratch_shapes=[pltpu.VMEM((n_col, height, size), jnp.float32)],
        name="round_two",
    )(tile_src, tile_dst, dist, code)
    fresh = lax.all_to_all(part, "col", 0, 0)
    distances, sums = pl.pallas_call(
        final_kernel,
        out_shape=(
            jax.ShapeDtypeStruct((height, size), jnp.float32),
            jax.ShapeDtypeStruct((1, height), jnp.float32),
        ),
        in_specs=[vmem, vmem],
        out_specs=(vmem, vmem),
        name="decode",
    )(fresh, own)
    other = lax.ppermute(sums, "rep", [(i, i ^ 1) for i in range(n_rep)])
    return distances, sums + other


def solution(mesh):
    cut = ("row", "col", "rep")
    return jax.shard_map(
        per_device,
        mesh=mesh,
        in_specs=(P(), P(cut, None, None), P(cut), P(cut), P(cut)),
        out_specs=(P(None, cut), P(("row", "col"), None)),
        check_vma=False,
    )
```

```python
import functools

import jax
import jax.numpy as jnp
from jax import lax
from jax.experimental import pallas as pl
from jax.experimental.pallas import tpu as pltpu
from jax.sharding import PartitionSpec as P

BLK_DEV = 1
STEP = 7.5
HALF = 63.0
FAR = 255.0
CHUNKS = 8


def relax(dist, edges, best):
    for q in range(dist.shape[0]):
        left = dist[q]
        for d in range(best.shape[0]):
            total = jnp.dot(left, edges[q, d], preferred_element_type=jnp.float32)
            best[d] = total if q == 0 else jnp.maximum(best[d], total)


def first_kernel(n_row, n_col, n_rep, sources, weights, src, dst, count, edges, hot, part, best, raw, ids, s_src, s_dst, sems, small):
    tiles, size, _ = raw.shape
    height = hot.shape[1]
    step = tiles // CHUNKS
    firsts = [
        pltpu.make_async_copy(a, b, small.at[i])
        for i, (a, b) in enumerate(((sources, ids), (src, s_src), (dst, s_dst)))
    ]
    for copy in firsts:
        copy.start()
    copies = [
        pltpu.make_async_copy(
            weights.at[pl.ds(c * step, step)], raw.at[pl.ds(c * step, step)], sems.at[c]
        )
        for c in range(CHUNKS)
    ]
    for copy in copies:
        copy.start()
    edges[...] = jnp.zeros_like(edges)
    for copy in firsts:
        copy.wait()
    col = lax.axis_index("col")
    wanted = jnp.broadcast_to(ids[...], (size, height)).T
    lane = lax.broadcasted_iota(jnp.int32, (height, size), 1)
    for q in range(n_row * n_rep):
        block = ((q // n_rep) * n_col + col) * n_rep + q % n_rep
        hot[q] = jnp.where(wanted == lane + block * size, 2.0**HALF, 0.0).astype(jnp.bfloat16)
    live = count[0]
    for c, copy in enumerate(copies):
        copy.wait()
        for k in range(c * step, (c + 1) * step):
            w = raw[k].astype(jnp.float32)
            bound = jnp.where(k < live, 0.5, 1e9)
            coded = jnp.where(w > bound, jnp.exp2(HALF - STEP * w), 0.0).astype(jnp.bfloat16)
            piece = s_src[k] // BLK_DEV
            q = piece // (n_col * n_rep) * n_rep + lax.rem(piece, n_rep)
            d = lax.rem(s_dst[k] // BLK_DEV // n_rep, n_col)
            edges[q, d] = jnp.maximum(edges[q, d], coded)
    relax(hot, edges, best)
    coded = (best[...] * 2.0**-HALF).astype(jnp.bfloat16)
    for r in range(n_row):
        part[r] = coded


def second_kernel(n_row, n_col, n_rep, mine, other, hot, edges, part, own, dist, best):
    rep = lax.axis_index("rep")
    for r in range(n_row):
        for p in range(n_rep):
            got = jnp.where(rep == p, jnp.max(mine[r], axis=0), jnp.max(other[r], axis=0))
            dist[r * n_rep + p] = jnp.maximum(got, hot[r * n_rep + p])
    own[...] = dist[lax.axis_index("row") * n_rep + rep]
    relax(dist, edges, best)
    part[...] = best[...].astype(jnp.bfloat16)


def final_kernel(fresh, own, distances, sums):
    best = jnp.max(fresh[...].astype(jnp.float32), axis=0)
    best = jnp.maximum(best, own[...].astype(jnp.float32) * 2.0**HALF)
    level = jnp.ceil((2 * HALF - 0.22 - jnp.log2(jnp.maximum(best, 2.0**-125))) / STEP)
    value = jnp.where(best > 0.0, level, FAR)
    distances[...] = jnp.where(value > 0.0, value, 0.0)
    inverse = jnp.where(value > 0.0, 1.0 / jnp.maximum(value, 1.0), 0.0)
    sums[...] = jnp.sum(inverse.T, axis=0, keepdims=True)


def in_hbm(array):
    return pltpu.with_memory_space_constraint(array, pltpu.HBM)


def per_device(sources, tile_weights, tile_src, tile_dst, tile_count):
    n_row, n_col, n_rep = (lax.axis_size(a) for a in ("row", "col", "rep"))
    height = sources.shape[0]
    tiles, size, _ = tile_weights.shape
    slots = n_row * n_rep
    vmem = pl.BlockSpec(memory_space=pltpu.VMEM)
    hbm = pl.BlockSpec(memory_space=pltpu.HBM)
    sizes = (n_row, n_col, n_rep)
    limit = pltpu.CompilerParams(vmem_limit_bytes=12 << 20)
    edges, hot, part = pl.pallas_call(
        functools.partial(first_kernel, *sizes),
        out_shape=(
            jax.ShapeDtypeStruct((slots, n_col, size, size), jnp.bfloat16),
            jax.ShapeDtypeStruct((slots, height, size), jnp.bfloat16),
            jax.ShapeDtypeStruct((n_row, n_col, height, size), jnp.bfloat16),
        ),
        in_specs=[hbm] * 4 + [pl.BlockSpec(memory_space=pltpu.SMEM)],
        out_specs=(vmem,) * 3,
        scratch_shapes=[
            pltpu.VMEM((n_col, height, size), jnp.float32),
            pltpu.VMEM((tiles, size, size), jnp.int32),
            pltpu.VMEM((1, height), jnp.int32),
            pltpu.SMEM((tiles,), jnp.int32),
            pltpu.SMEM((tiles,), jnp.int32),
            pltpu.SemaphoreType.DMA((CHUNKS,)),
            pltpu.SemaphoreType.DMA((3,)),
        ],
        compiler_params=limit,
        name="round_one",
    )(*map(in_hbm, (sources.reshape(1, height), tile_weights, tile_src, tile_dst)), tile_count)
    mine = lax.all_to_all(
        part.reshape(n_row * n_col, height, size), ("row", "col"), 0, 0
    ).reshape(n_row, n_col, height, size)
    other = lax.ppermute(mine, "rep", [(i, (i + 1) % n_rep) for i in range(n_rep)])
    part, own = pl.pallas_call(
        functools.partial(second_kernel, *sizes),
        out_shape=(
            jax.ShapeDtypeStruct((n_col, height, size), jnp.bfloat16),
            jax.ShapeDtypeStruct((height, size), jnp.bfloat16),
        ),
        in_specs=[vmem] * 4,
        out_specs=(vmem,) * 2,
        scratch_shapes=[
            pltpu.VMEM((slots, height, size), jnp.bfloat16),
            pltpu.VMEM((n_col, height, size), jnp.float32),
        ],
        compiler_params=limit,
        name="round_two",
    )(mine, other, hot, edges)
    fresh = lax.all_to_all(part, "col", 0, 0)
    distances, sums = pl.pallas_call(
        final_kernel,
        out_shape=(
            jax.ShapeDtypeStruct((height, size), jnp.float32),
            jax.ShapeDtypeStruct((1, height), jnp.float32),
        ),
        in_specs=[vmem, vmem],
        out_specs=(vmem, vmem),
        compiler_params=limit,
        name="decode",
    )(fresh, own)
    other = lax.ppermute(sums, "rep", [(i, (i + 1) % n_rep) for i in range(n_rep)])
    return distances, sums + other


def solution(mesh):
    cut = ("row", "col", "rep")
    return jax.shard_map(
        per_device,
        mesh=mesh,
        in_specs=(P(), P(cut, None, None), P(cut), P(cut), P(cut)),
        out_specs=(P(None, cut), P(("row", "col"), None)),
        check_vma=False,
    )
```

```python
import functools

import jax
import jax.numpy as jnp
from jax import lax
from jax.experimental import pallas as pl
from jax.experimental.pallas import tpu as pltpu
from jax.sharding import PartitionSpec as P

BLK_DEV = 1
STEP = 7.5
HALF = 63.0
FAR = 255.0
CHUNKS = 8
F32, BF16 = jnp.float32, jnp.bfloat16


def relax(dist, edges, best):
    for q in range(dist.shape[0]):
        left = dist[q]
        for d in range(best.shape[0]):
            total = jnp.dot(left, edges[q, d], preferred_element_type=F32)
            best[d] = total if q == 0 else jnp.maximum(best[d], total)


def column_of(vertex, size, n_col, n_rep):
    shift = (size * BLK_DEV * n_rep).bit_length() - 1
    return lax.shift_right_logical(vertex, shift) & (n_col - 1)


def spread(part, best):
    coded = (best[...] * 2.0**-HALF).astype(BF16)
    for r in range(part.shape[0]):
        part[r] = coded


def first_kernel(
    sizes, sources, weights, src, dst, count,
    edges, hot, pick, part, over,
    few, best, raw, ids, s_src, s_dst, sems, small,
):
    n_row, n_col, n_rep = sizes
    tiles, size, _ = raw.shape
    height, room = hot.shape[1], few.shape[1]
    step = tiles // CHUNKS
    firsts = [
        pltpu.make_async_copy(a, b, small.at[i])
        for i, (a, b) in enumerate(((sources, ids), (src, s_src), (dst, s_dst)))
    ]
    for copy in firsts:
        copy.start()
    copies = [
        pltpu.make_async_copy(
            weights.at[pl.ds(c * step, step)], raw.at[pl.ds(c * step, step)], sems.at[c]
        )
        for c in range(CHUNKS)
    ]
    for copy in copies:
        copy.start()
    edges[...] = jnp.zeros_like(edges)
    for copy in firsts:
        copy.wait()
    me = lax.axis_index("col")
    along = jnp.broadcast_to(ids[...], (size, height))
    down = along.T
    lane = lax.broadcasted_iota(jnp.int32, (height, size), 1)
    col_along = column_of(along[:height], size, n_col, n_rep)
    col_down = column_of(down, size, n_col, n_rep)
    s_a = lax.broadcasted_iota(jnp.int32, (height, height), 1)
    s_d = lax.broadcasted_iota(jnp.int32, (height, height), 0)
    same = col_along == col_down[:, :height]
    rank_down = jnp.sum(jnp.where(same & (s_a < s_d), 1.0, 0.0), axis=1, keepdims=True)
    rank_along = jnp.sum(jnp.where(same & (s_d < s_a), 1.0, 0.0), axis=0, keepdims=True)
    over[0] = (jnp.max(rank_along) >= room).astype(jnp.int32)
    place = lax.broadcasted_iota(jnp.int32, (height, n_col * room), 1)
    slot = jnp.where(rank_down < room, rank_down + room * col_down[:, :1].astype(F32), -1.0)
    pick[...] = jnp.where(place.astype(F32) == slot, 1.0, 0.0).astype(BF16)
    order = lax.broadcasted_iota(jnp.int32, (room, height), 0).astype(F32)
    taken = (order == rank_along) & (col_along[:room] == me)
    vertex = jnp.sum(jnp.where(taken, along[:room].astype(F32) + 1.0, 0.0), axis=1, keepdims=True) - 1.0
    for q in range(n_row * n_rep):
        at = lane + (((q // n_rep) * n_col + me) * n_rep + q % n_rep) * size
        hot[q] = jnp.where(down == at, 2.0**HALF, 0.0).astype(BF16)
        few[q] = jnp.where(vertex == at[:room].astype(F32), 2.0**HALF, 0.0).astype(BF16)
    live = count[0]
    for c, copy in enumerate(copies):
        copy.wait()
        for k in range(c * step, (c + 1) * step):
            w = raw[k].astype(F32).astype(BF16)
            bound = jnp.where(k < live, 0.5, 1e9).astype(BF16)
            coded = jnp.where(w > bound, jnp.exp2(BF16(HALF) - BF16(STEP) * w), BF16(0.0))
            piece = s_src[k] // BLK_DEV
            q = piece // (n_col * n_rep) * n_rep + lax.rem(piece, n_rep)
            d = lax.rem(s_dst[k] // BLK_DEV // n_rep, n_col)
            edges[q, d] = jnp.maximum(edges[q, d], coded)
    relax(few, edges, best)
    spread(part, best)


def first_kernel_all(hot, edges, part, best):
    relax(hot, edges, best)
    spread(part, best)


def second_kernel(sizes, packed, mine, other, hot, pick, edges, part, own, dist, best):
    n_row, n_col, n_rep = sizes
    rep = lax.axis_index("rep")
    for r in range(n_row):
        got = []
        for side in (mine, other):
            rows = side[r]
            if packed:
                rows = rows.reshape(-1, rows.shape[-1])
                got.append(jnp.dot(pick[...], rows, preferred_element_type=F32).astype(BF16))
            else:
                got.append(jnp.max(rows, axis=0))
        for p in range(n_rep):
            q = r * n_rep + p
            dist[q] = jnp.maximum(jnp.where(rep == p, got[0], got[1]), hot[q])
    own[...] = dist[lax.axis_index("row") * n_rep + rep]
    relax(dist, edges, best)
    part[...] = best[...].astype(BF16)


def final_kernel(fresh, own, distances, sums):
    best = jnp.max(fresh[...].astype(F32), axis=0)
    best = jnp.maximum(best, own[...].astype(F32) * 2.0**HALF)
    level = jnp.ceil((2 * HALF - 0.22 - jnp.log2(jnp.maximum(best, 2.0**-125))) / STEP)
    value = jnp.where(best > 0.0, level, FAR)
    distances[...] = jnp.where(value > 0.0, value, 0.0)
    inverse = jnp.where(value > 0.0, 1.0 / jnp.maximum(value, 1.0), 0.0)
    sums[...] = jnp.sum(inverse.T, axis=0, keepdims=True)


def in_hbm(array):
    return pltpu.with_memory_space_constraint(array, pltpu.HBM)


def per_device(sources, tile_weights, tile_src, tile_dst, tile_count):
    sizes = n_row, n_col, n_rep = tuple(lax.axis_size(a) for a in ("row", "col", "rep"))
    height = sources.shape[0]
    tiles, size, _ = tile_weights.shape
    slots = n_row * n_rep
    room = min(height, max(16, 2 * height // n_col))
    assert n_rep == 2 and all(n & (n - 1) == 0 for n in (*sizes, size))
    vmem = pl.BlockSpec(memory_space=pltpu.VMEM)
    smem = pl.BlockSpec(memory_space=pltpu.SMEM)
    hbm = pl.BlockSpec(memory_space=pltpu.HBM)
    limit = pltpu.CompilerParams(vmem_limit_bytes=14 << 20)
    shape = jax.ShapeDtypeStruct
    swap = [(i, (i + 1) % n_rep) for i in range(n_rep)]
    best = pltpu.VMEM((n_col, height, size), F32)
    edges, hot, pick, part, over = pl.pallas_call(
        functools.partial(first_kernel, sizes),
        out_shape=(
            shape((slots, n_col, size, size), BF16),
            shape((slots, height, size), BF16),
            shape((height, n_col * room), BF16),
            shape((n_row, n_col, room, size), BF16),
            pltpu.SMEM((1,), jnp.int32),
        ),
        in_specs=[hbm] * 4 + [smem],
        out_specs=(vmem,) * 4 + (smem,),
        scratch_shapes=[
            pltpu.VMEM((slots, room, size), BF16),
            pltpu.VMEM((n_col, room, size), F32),
            pltpu.VMEM((tiles, size, size), jnp.int32),
            pltpu.VMEM((1, height), jnp.int32),
            pltpu.SMEM((tiles,), jnp.int32),
            pltpu.SMEM((tiles,), jnp.int32),
            pltpu.SemaphoreType.DMA((CHUNKS,)),
            pltpu.SemaphoreType.DMA((3,)),
        ],
        compiler_params=limit,
        name="round_one",
    )(*map(in_hbm, (sources.reshape(1, height), tile_weights, tile_src, tile_dst)), tile_count)

    def finish(packed, part, hot, pick, edges):
        mine = lax.all_to_all(
            part.reshape(n_row * n_col, *part.shape[2:]), ("row", "col"), 0, 0
        ).reshape(part.shape)
        other = lax.ppermute(mine, "rep", swap)
        return pl.pallas_call(
            functools.partial(second_kernel, sizes, packed),
            out_shape=(shape((n_col, height, size), BF16), shape((height, size), BF16)),
            in_specs=[vmem] * 5,
            out_specs=(vmem,) * 2,
            scratch_shapes=[pltpu.VMEM((slots, height, size), BF16), best],
            compiler_params=limit,
            name="round_two" if packed else "round_two_all",
        )(mine, other, hot, pick, edges)

    def common(part, hot, pick, edges):
        return finish(True, part, hot, pick, edges)

    def crowded(part, hot, pick, edges):
        full = pl.pallas_call(
            first_kernel_all,
            out_shape=shape((n_row, n_col, height, size), BF16),
            in_specs=[vmem] * 2,
            out_specs=vmem,
            scratch_shapes=[best],
            compiler_params=limit,
            name="round_one_all",
        )(hot, edges)
        return finish(False, full, hot, pick, edges)

    part, own = lax.cond(over[0] > 0, crowded, common, part, hot, pick, edges)
    fresh = lax.all_to_all(part, "col", 0, 0)
    distances, sums = pl.pallas_call(
        final_kernel,
        out_shape=(pltpu.VMEM((height, size), F32), shape((1, height), F32)),
        in_specs=[vmem, vmem],
        out_specs=(vmem, vmem),
        compiler_params=limit,
        name="decode",
    )(fresh, own)
    return distances, sums + lax.ppermute(sums, "rep", swap)


def solution(mesh):
    cut = ("row", "col", "rep")
    return jax.shard_map(
        per_device,
        mesh=mesh,
        in_specs=(P(), P(cut, None, None), P(cut), P(cut), P(cut)),
        out_specs=(P(None, cut), P(("row", "col"), None)),
        check_vma=False,
    )
```

```python
import functools

import jax
import jax.numpy as jnp
from jax import lax
from jax.experimental import pallas as pl
from jax.experimental.pallas import tpu as pltpu
from jax.sharding import PartitionSpec as P

BLK_DEV = 1
STEP = 7.5
TOP = 126.0
FAR = 255.0
CHUNKS = 4
F32, BF16 = jnp.float32, jnp.bfloat16


def relax(dist, code, q_of, d_of, best, tiles):
    for k in tiles:
        total = jnp.dot(dist[q_of[k]], code[k], preferred_element_type=F32)
        d = d_of[k]
        best[d] = jnp.maximum(best[d], total)


def log(n):
    return n.bit_length() - 1


def column_of(vertex, size, n_col, n_rep):
    return lax.shift_right_logical(vertex, log(size * n_rep)) & (n_col - 1)


def spread(part, best):
    coded = best[: part.shape[1]].astype(BF16)
    for r in range(part.shape[0]):
        part[r] = coded


def first_kernel(
    sizes, sources, weights, src, dst, count,
    code, hot, pick, part, over, q_of, d_of,
    few, best, raw, ids, s_src, s_dst, sems, small,
):
    n_row, n_col, n_rep = sizes
    tiles, size, _ = raw.shape
    height, room = hot.shape[1], few.shape[1]
    step = tiles // CHUNKS
    firsts = [
        pltpu.make_async_copy(a, b, small.at[i])
        for i, (a, b) in enumerate(((sources, ids), (src, s_src), (dst, s_dst)))
    ]
    for copy in firsts:
        copy.start()
    copies = [
        pltpu.make_async_copy(
            weights.at[pl.ds(c * step, step)], raw.at[pl.ds(c * step, step)], sems.at[c]
        )
        for c in range(CHUNKS)
    ]
    for copy in copies:
        copy.start()
    best[...] = jnp.zeros_like(best)
    for copy in firsts:
        copy.wait()
    me = lax.axis_index("col")
    along = jnp.broadcast_to(ids[...], (size, height))
    down = along.T
    lane = lax.broadcasted_iota(jnp.int32, (height, size), 1)
    col_along = column_of(along[:height], size, n_col, n_rep)
    col_down = column_of(down, size, n_col, n_rep)
    s_a = lax.broadcasted_iota(jnp.int32, (height, height), 1)
    s_d = lax.broadcasted_iota(jnp.int32, (height, height), 0)
    same = col_along == col_down[:, :height]
    rank_down = jnp.sum(jnp.where(same & (s_a < s_d), 1.0, 0.0), axis=1, keepdims=True)
    rank_along = jnp.sum(jnp.where(same & (s_d < s_a), 1.0, 0.0), axis=0, keepdims=True)
    over[0] = (jnp.max(rank_along) >= room).astype(jnp.int32)
    place = lax.broadcasted_iota(jnp.int32, (height, n_col * room), 1)
    slot = jnp.where(rank_down < room, rank_down + room * col_down[:, :1].astype(F32), -1.0)
    pick[...] = jnp.where(place.astype(F32) == slot, 1.0, 0.0).astype(BF16)
    order = lax.broadcasted_iota(jnp.int32, (room, height), 0).astype(F32)
    taken = (order == rank_along) & (col_along[:room] == me)
    vertex = jnp.sum(jnp.where(taken, along[:room].astype(F32) + 1.0, 0.0), axis=1, keepdims=True) - 1.0
    for q in range(n_row * n_rep):
        at = lane + (((q // n_rep) * n_col + me) * n_rep + q % n_rep) * size
        hot[q] = jnp.where(down == at, 2.0**TOP, 0.0).astype(BF16)
        few[q] = jnp.where(vertex == at[:room].astype(F32), 2.0**TOP, 0.0).astype(BF16)
    live = count[0]
    for k in range(tiles):
        q_of[k] = lax.shift_right_logical(s_src[k], log(n_col * n_rep)) * n_rep + (s_src[k] & (n_rep - 1))
        d = lax.shift_right_logical(s_dst[k], log(n_rep)) & (n_col - 1)
        d_of[k] = jnp.where(k < live, d, n_col)
    for c, copy in enumerate(copies):
        copy.wait()
        mine = range(c * step, (c + 1) * step)
        for k in mine:
            w = raw[k].astype(F32).astype(BF16)
            code[k] = jnp.where(w > 0, jnp.exp2(BF16(-STEP) * w), BF16(0.0))
    relax(few, code, q_of, d_of, best, range(tiles))
    spread(part, best)


def first_kernel_all(hot, code, q_of, d_of, part, best):
    best[...] = jnp.zeros_like(best)
    relax(hot, code, q_of, d_of, best, range(code.shape[0]))
    spread(part, best)


def second_kernel(sizes, packed, mine, other, hot, pick, code, q_of, d_of, part, own, dist, best):
    n_row, n_col, n_rep = sizes
    rep = lax.axis_index("rep")
    for r in range(n_row):
        got = []
        for side in (mine, other):
            rows = side[r]
            if packed:
                rows = rows.reshape(-1, rows.shape[-1])
                got.append(jnp.dot(pick[...], rows, preferred_element_type=F32).astype(BF16))
            else:
                got.append(jnp.max(rows, axis=0))
        for p in range(n_rep):
            q = r * n_rep + p
            dist[q] = jnp.maximum(jnp.where(rep == p, got[0], got[1]), hot[q])
    own[...] = dist[lax.axis_index("row") * n_rep + rep]
    best[...] = jnp.zeros_like(best)
    relax(dist, code, q_of, d_of, best, range(code.shape[0]))
    part[...] = best[:n_col].astype(BF16)


def final_kernel(fresh, own, distances, sums):
    best = jnp.max(fresh[...].astype(F32), axis=0)
    best = jnp.maximum(best, own[...].astype(F32))
    level = jnp.ceil((TOP - 0.22 - jnp.log2(jnp.maximum(best, 2.0**-125))) / STEP)
    value = jnp.where(best > 0.0, level, FAR)
    distances[...] = jnp.where(value > 0.0, value, 0.0)
    inverse = jnp.where(value > 0.0, 1.0 / jnp.maximum(value, 1.0), 0.0)
    sums[...] = jnp.sum(inverse.T, axis=0, keepdims=True)


def in_hbm(array):
    return pltpu.with_memory_space_constraint(array, pltpu.HBM)


def per_device(sources, tile_weights, tile_src, tile_dst, tile_count):
    sizes = n_row, n_col, n_rep = tuple(lax.axis_size(a) for a in ("row", "col", "rep"))
    height = sources.shape[0]
    tiles, size, _ = tile_weights.shape
    slots = n_row * n_rep
    room = min(height, max(16, 2 * height // n_col))
    assert n_rep == 2 and all(n & (n - 1) == 0 for n in (*sizes, size))
    vmem = pl.BlockSpec(memory_space=pltpu.VMEM)
    smem = pl.BlockSpec(memory_space=pltpu.SMEM)
    hbm = pl.BlockSpec(memory_space=pltpu.HBM)
    limit = pltpu.CompilerParams(vmem_limit_bytes=14 << 20)
    shape = jax.ShapeDtypeStruct
    swap = [(i, (i + 1) % n_rep) for i in range(n_rep)]
    best = pltpu.VMEM((n_col + 1, height, size), F32)
    code, hot, pick, part, over, *places = pl.pallas_call(
        functools.partial(first_kernel, sizes),
        out_shape=(
            shape((tiles, size, size), BF16),
            shape((slots, height, size), BF16),
            shape((height, n_col * room), BF16),
            shape((n_row, n_col, room, size), BF16),
            pltpu.SMEM((1,), jnp.int32),
            pltpu.SMEM((tiles,), jnp.int32),
            pltpu.SMEM((tiles,), jnp.int32),
        ),
        in_specs=[hbm] * 4 + [smem],
        out_specs=(vmem,) * 4 + (smem,) * 3,
        scratch_shapes=[
            pltpu.VMEM((slots, room, size), BF16),
            pltpu.VMEM((n_col + 1, room, size), F32),
            pltpu.VMEM((tiles, size, size), jnp.int32),
            pltpu.VMEM((1, height), jnp.int32),
            pltpu.SMEM((tiles,), jnp.int32),
            pltpu.SMEM((tiles,), jnp.int32),
            pltpu.SemaphoreType.DMA((CHUNKS,)),
            pltpu.SemaphoreType.DMA((3,)),
        ],
        compiler_params=limit,
        name="round_one",
    )(*map(in_hbm, (sources.reshape(1, height), tile_weights, tile_src, tile_dst)), tile_count)

    def finish(packed, part, hot, pick, code, *places):
        mine = lax.all_to_all(
            part.reshape(n_row * n_col, *part.shape[2:]), ("row", "col"), 0, 0
        ).reshape(part.shape)
        other = lax.ppermute(mine, "rep", swap)
        return pl.pallas_call(
            functools.partial(second_kernel, sizes, packed),
            out_shape=(shape((n_col, height, size), BF16), shape((height, size), BF16)),
            in_specs=[vmem] * 5 + [smem] * 2,
            out_specs=(vmem,) * 2,
            scratch_shapes=[pltpu.VMEM((slots, height, size), BF16), best],
            compiler_params=limit,
            name="round_two" if packed else "round_two_all",
        )(mine, other, hot, pick, code, *places)

    def common(part, hot, pick, code, *places):
        return finish(True, part, hot, pick, code, *places)

    def crowded(part, hot, pick, code, *places):
        full = pl.pallas_call(
            first_kernel_all,
            out_shape=shape((n_row, n_col, height, size), BF16),
            in_specs=[vmem] * 2 + [smem] * 2,
            out_specs=vmem,
            scratch_shapes=[best],
            compiler_params=limit,
            name="round_one_all",
        )(hot, code, *places)
        return finish(False, full, hot, pick, code, *places)

    part, own = lax.cond(over[0] > 0, crowded, common, part, hot, pick, code, *places)
    fresh = lax.all_to_all(part, "col", 0, 0)
    distances, sums = pl.pallas_call(
        final_kernel,
        out_shape=(pltpu.VMEM((height, size), F32), shape((1, height), F32)),
        in_specs=[vmem, vmem],
        out_specs=(vmem, vmem),
        compiler_params=limit,
        name="decode",
    )(fresh, own)
    return distances, sums + lax.ppermute(sums, "rep", swap)


def solution(mesh):
    cut = ("row", "col", "rep")
    return jax.shard_map(
        per_device,
        mesh=mesh,
        in_specs=(P(), P(cut, None, None), P(cut), P(cut), P(cut)),
        out_specs=(P(None, cut), P(("row", "col"), None)),
        check_vma=False,
    )
```

```python
import functools

import jax
import jax.numpy as jnp
from jax import lax
from jax.experimental import pallas as pl
from jax.experimental.pallas import tpu as pltpu
from jax.sharding import PartitionSpec as P

BLK_DEV = 1
STEP = 7.5
TOP = 126.0
FAR = 255.0
CHUNKS = 4
F32, BF16 = jnp.float32, jnp.bfloat16


def relax(dist, edges, best):
    width = best.shape[0]
    for q, left in enumerate(dist):
        for d in range(width):
            total = jnp.dot(left, edges[q * width + d], preferred_element_type=F32)
            best[d] = jnp.maximum(best[d], total) if q else total


def log(n):
    return n.bit_length() - 1


def column_of(vertex, size, n_col, n_rep):
    return lax.shift_right_logical(vertex, log(size * n_rep)) & (n_col - 1)


def spread(part, best):
    coded = best[...].astype(BF16)
    for r in range(part.shape[0]):
        part[r] = coded


def first_kernel(
    sizes, sources, weights, src, dst, count,
    edges, hot, pick, part, over,
    few, best, raw, ids, s_src, s_dst, sems, small,
):
    n_row, n_col, n_rep = sizes
    tiles, size, _ = raw.shape
    height, room = hot.shape[1], few.shape[1]
    step = tiles // CHUNKS
    firsts = [
        pltpu.make_async_copy(a, b, small.at[i])
        for i, (a, b) in enumerate(((sources, ids), (src, s_src), (dst, s_dst)))
    ]
    for copy in firsts:
        copy.start()
    copies = [
        pltpu.make_async_copy(
            weights.at[pl.ds(c * step, step)], raw.at[pl.ds(c * step, step)], sems.at[c]
        )
        for c in range(CHUNKS)
    ]
    for copy in copies:
        copy.start()
    edges[...] = jnp.zeros_like(edges)
    for copy in firsts:
        copy.wait()
    me = lax.axis_index("col")
    along = jnp.broadcast_to(ids[...], (size, height))
    down = along.T
    lane = lax.broadcasted_iota(jnp.int32, (height, size), 1)
    col_along = column_of(along[:height], size, n_col, n_rep)
    col_down = column_of(down, size, n_col, n_rep)
    s_a = lax.broadcasted_iota(jnp.int32, (height, height), 1)
    s_d = lax.broadcasted_iota(jnp.int32, (height, height), 0)
    same = col_along == col_down[:, :height]
    rank_down = jnp.sum(jnp.where(same & (s_a < s_d), 1.0, 0.0), axis=1, keepdims=True)
    rank_along = jnp.sum(jnp.where(same & (s_d < s_a), 1.0, 0.0), axis=0, keepdims=True)
    over[0] = (jnp.max(rank_along) >= room).astype(jnp.int32)
    place = lax.broadcasted_iota(jnp.int32, (height, n_col * room), 1)
    slot = jnp.where(rank_down < room, rank_down + room * col_down[:, :1].astype(F32), -1.0)
    pick[...] = jnp.where(place.astype(F32) == slot, 1.0, 0.0).astype(BF16)
    order = lax.broadcasted_iota(jnp.int32, (room, height), 0).astype(F32)
    taken = (order == rank_along) & (col_along[:room] == me)
    vertex = jnp.sum(jnp.where(taken, along[:room].astype(F32) + 1.0, 0.0), axis=1, keepdims=True) - 1.0
    rep = lax.axis_index("rep")
    for q in range(n_row * n_rep):
        at = lane + ((q % n_row * n_col + me) * n_rep + (rep ^ (q // n_row))) * size
        hot[q] = jnp.where(down == at, 2.0**TOP, 0.0).astype(BF16)
        few[q] = jnp.where(vertex == at[:room].astype(F32), 2.0**TOP, 0.0).astype(BF16)
    live = count[0]
    for c, copy in enumerate(copies):
        copy.wait()
        for k in range(c * step, (c + 1) * step):
            q = ((s_src[k] & 1) ^ rep) * n_row + lax.shift_right_logical(s_src[k], log(n_col * n_rep))
            d = lax.shift_right_logical(s_dst[k], log(n_rep)) & (n_col - 1)
            at = jnp.where(k < live, q * n_col + d, n_row * n_rep * n_col)
            w = raw[k].astype(F32).astype(BF16)
            coded = jnp.where(w > 0, jnp.exp2(BF16(-STEP) * w), BF16(0.0))
            edges[at] = jnp.maximum(edges[at], coded)
    relax([few[q] for q in range(n_row * n_rep)], edges, best)
    spread(part, best)


def first_kernel_all(hot, edges, part, best):
    relax([hot[q] for q in range(hot.shape[0])], edges, best)
    spread(part, best)


def second_kernel(sizes, packed, got, hot, pick, edges, theirs, part, own, best):
    n_row, n_col, n_rep = sizes
    dist = []
    for r in range(n_row):
        if packed:
            rows = got[r].reshape(-1, got.shape[-1])
            value = jnp.dot(pick[...], rows, preferred_element_type=F32).astype(BF16)
        else:
            value = jnp.max(got[r], axis=0)
        dist.append(jnp.maximum(value, hot[r]))
    here = lax.axis_index("row")
    value = dist[0]
    for r in range(1, n_row):
        value = jnp.where(here == r, dist[r], value)
    own[...] = value
    relax(dist, edges, best)
    part[:, 0] = best[...].astype(BF16)
    relax(dist, theirs.at[pl.ds(n_row * n_col, n_row * n_col)], best)
    part[:, 1] = best[...].astype(BF16)


def merge_kernel(fresh, own, merged):
    merged[0] = jnp.maximum(jnp.max(fresh[:, 0], axis=0), own[...])
    merged[1] = jnp.max(fresh[:, 1], axis=0)


def decode(code):
    code = code.astype(F32)
    level = jnp.ceil((TOP - 0.22 - jnp.log2(jnp.maximum(code, 2.0**-125))) / STEP)
    value = jnp.where(code > 0.0, level, FAR)
    return jnp.where(value > 0.0, value, 0.0)


def final_kernel(mine, theirs, distances, sums):
    value = decode(jnp.maximum(mine[0], theirs[1]))
    other = decode(jnp.maximum(mine[1], theirs[0]))
    distances[...] = value
    inverse = jnp.where(value > 0.0, 1.0 / jnp.maximum(value, 1.0), 0.0)
    inverse += jnp.where(other > 0.0, 1.0 / jnp.maximum(other, 1.0), 0.0)
    sums[...] = jnp.sum(inverse.T, axis=0, keepdims=True)


def in_hbm(array):
    return pltpu.with_memory_space_constraint(array, pltpu.HBM)


def per_device(sources, tile_weights, tile_src, tile_dst, tile_count):
    sizes = n_row, n_col, n_rep = tuple(lax.axis_size(a) for a in ("row", "col", "rep"))
    height = sources.shape[0]
    tiles, size, _ = tile_weights.shape
    slots = n_row * n_rep
    room = min(height, max(16, 2 * height // n_col))
    assert n_rep == 2 and all(n & (n - 1) == 0 for n in (*sizes, size))
    vmem = pl.BlockSpec(memory_space=pltpu.VMEM)
    smem = pl.BlockSpec(memory_space=pltpu.SMEM)
    hbm = pl.BlockSpec(memory_space=pltpu.HBM)
    limit = pltpu.CompilerParams(vmem_limit_bytes=28 << 20)
    shape = jax.ShapeDtypeStruct
    swap = [(i, (i + 1) % n_rep) for i in range(n_rep)]
    places = slots * n_col + 1
    best = pltpu.VMEM((n_col, height, size), F32)
    edges, hot, pick, part, over = pl.pallas_call(
        functools.partial(first_kernel, sizes),
        out_shape=(
            shape((places, size, size), BF16),
            shape((slots, height, size), BF16),
            shape((height, n_col * room), BF16),
            shape((n_row, n_col, room, size), BF16),
            pltpu.SMEM((1,), jnp.int32),
        ),
        in_specs=[hbm] * 4 + [smem],
        out_specs=(vmem,) * 4 + (smem,),
        scratch_shapes=[
            pltpu.VMEM((slots, room, size), BF16),
            pltpu.VMEM((n_col, room, size), F32),
            pltpu.VMEM((tiles, size, size), jnp.int32),
            pltpu.VMEM((1, height), jnp.int32),
            pltpu.SMEM((tiles,), jnp.int32),
            pltpu.SMEM((tiles,), jnp.int32),
            pltpu.SemaphoreType.DMA((CHUNKS,)),
            pltpu.SemaphoreType.DMA((3,)),
        ],
        compiler_params=limit,
        name="round_one",
    )(*map(in_hbm, (sources.reshape(1, height), tile_weights, tile_src, tile_dst)), tile_count)

    def finish(packed, part, hot, pick, edges):
        theirs = lax.ppermute(edges, "rep", swap)
        got = lax.all_to_all(
            part.reshape(n_row * n_col, *part.shape[2:]), ("row", "col"), 0, 0
        ).reshape(part.shape)
        return pl.pallas_call(
            functools.partial(second_kernel, sizes, packed),
            out_shape=(shape((n_col, n_rep, height, size), BF16), shape((height, size), BF16)),
            in_specs=[vmem] * 5,
            out_specs=(vmem,) * 2,
            scratch_shapes=[best],
            compiler_params=limit,
            name="round_two" if packed else "round_two_all",
        )(got, hot, pick, edges, theirs)

    def common(part, hot, pick, edges):
        return finish(True, part, hot, pick, edges)

    def crowded(part, hot, pick, edges):
        full = pl.pallas_call(
            first_kernel_all,
            out_shape=shape((n_row, n_col, height, size), BF16),
            in_specs=[vmem] * 2,
            out_specs=vmem,
            scratch_shapes=[best],
            compiler_params=limit,
            name="round_one_all",
        )(hot, edges)
        return finish(False, full, hot, pick, edges)

    part, own = lax.cond(over[0] > 0, crowded, common, part, hot, pick, edges)
    fresh = lax.all_to_all(part, "col", 0, 0)
    mine = pl.pallas_call(
        merge_kernel,
        out_shape=shape((n_rep, height, size), BF16),
        in_specs=[vmem] * 2,
        out_specs=vmem,
        compiler_params=limit,
        name="merge",
    )(fresh, own)
    theirs = lax.ppermute(mine, "rep", swap)
    return pl.pallas_call(
        final_kernel,
        out_shape=(shape((height, size), F32), shape((1, height), F32)),
        in_specs=[vmem] * 2,
        out_specs=(vmem,) * 2,
        compiler_params=limit,
        name="decode",
    )(mine, theirs)


def solution(mesh):
    cut = ("row", "col", "rep")
    return jax.shard_map(
        per_device,
        mesh=mesh,
        in_specs=(P(), P(cut, None, None), P(cut), P(cut), P(cut)),
        out_specs=(P(None, cut), P(("row", "col"), None)),
        check_vma=False,
    )
```

```python
import functools

import jax
import jax.numpy as jnp
from jax import lax
from jax.experimental import pallas as pl
from jax.experimental.pallas import tpu as pltpu
from jax.sharding import PartitionSpec as P

BLK_DEV = 1
STEP = 7.5
TOP = 126.0
FAR = 255.0
CHUNKS = 4
F32, BF16 = jnp.float32, jnp.bfloat16


def relax(dist, edges, best):
    width = best.shape[0]
    for q, left in enumerate(dist):
        for d in range(width):
            total = jnp.dot(left, edges[q * width + d], preferred_element_type=F32)
            best[d] = jnp.maximum(best[d], total) if q else total


def log(n):
    return n.bit_length() - 1


def column_of(vertex, size, n_col, n_rep):
    return lax.shift_right_logical(vertex, log(size * n_rep)) & (n_col - 1)


def spread(part, best):
    coded = best[...].astype(BF16)
    for r in range(part.shape[0]):
        part[r] = coded


def first_kernel(
    sizes, sources, weights, src, dst, count,
    edges, hot, pick, part, over,
    few, best, raw, ids, s_src, s_dst, sems, small,
):
    n_row, n_col, n_rep = sizes
    tiles, size, _ = raw.shape
    height, room = hot.shape[1], few.shape[1]
    step = tiles // CHUNKS
    firsts = [
        pltpu.make_async_copy(a, b, small.at[i])
        for i, (a, b) in enumerate(((sources, ids), (src, s_src), (dst, s_dst)))
    ]
    for copy in firsts:
        copy.start()
    copies = [
        pltpu.make_async_copy(
            weights.at[pl.ds(c * step, step)], raw.at[pl.ds(c * step, step)], sems.at[c]
        )
        for c in range(CHUNKS)
    ]
    for copy in copies:
        copy.start()
    edges[...] = jnp.zeros_like(edges)
    for copy in firsts:
        copy.wait()
    me = lax.axis_index("col")
    along = jnp.broadcast_to(ids[...], (size, height))
    down = along.T
    lane = lax.broadcasted_iota(jnp.int32, (height, size), 1)
    col_along = column_of(along[:height], size, n_col, n_rep)
    col_down = column_of(down, size, n_col, n_rep)
    s_a = lax.broadcasted_iota(jnp.int32, (height, height), 1)
    s_d = lax.broadcasted_iota(jnp.int32, (height, height), 0)
    same = col_along == col_down[:, :height]
    rank_down = jnp.sum(jnp.where(same & (s_a < s_d), 1.0, 0.0), axis=1, keepdims=True)
    rank_along = jnp.sum(jnp.where(same & (s_d < s_a), 1.0, 0.0), axis=0, keepdims=True)
    over[0] = (jnp.max(rank_along) >= room).astype(jnp.int32)
    place = lax.broadcasted_iota(jnp.int32, (height, n_col * room), 1)
    slot = jnp.where(rank_down < room, rank_down + room * col_down[:, :1].astype(F32), -1.0)
    pick[...] = jnp.where(place.astype(F32) == slot, 1.0, 0.0).astype(BF16)
    order = lax.broadcasted_iota(jnp.int32, (room, height), 0).astype(F32)
    taken = (order == rank_along) & (col_along[:room] == me)
    vertex = jnp.sum(jnp.where(taken, along[:room].astype(F32) + 1.0, 0.0), axis=1, keepdims=True) - 1.0
    rep = lax.axis_index("rep")
    for q in range(n_row * n_rep):
        at = lane + ((q % n_row * n_col + me) * n_rep + (rep ^ (q // n_row))) * size
        hot[q] = jnp.where(down == at, 2.0**TOP, 0.0).astype(BF16)
        few[q] = jnp.where(vertex == at[:room].astype(F32), 2.0**TOP, 0.0).astype(BF16)
    live = count[0]
    for c, copy in enumerate(copies):
        copy.wait()
        for k in range(c * step, (c + 1) * step):
            q = ((s_src[k] & 1) ^ rep) * n_row + lax.shift_right_logical(s_src[k], log(n_col * n_rep))
            d = lax.shift_right_logical(s_dst[k], log(n_rep)) & (n_col - 1)
            at = jnp.where(k < live, q * n_col + d, n_row * n_rep * n_col)
            w = raw[k].astype(F32).astype(BF16)
            coded = jnp.where(w > 0, jnp.exp2(BF16(-STEP) * w), BF16(0.0))
            edges[at] = jnp.maximum(edges[at], coded)
    relax([few[q] for q in range(n_row * n_rep)], edges, best)
    spread(part, best)


def first_kernel_all(hot, edges, part, best):
    relax([hot[q] for q in range(hot.shape[0])], edges, best)
    spread(part, best)


def second_kernel(sizes, packed, got, hot, pick, edges, theirs, part, own, best):
    n_row, n_col, n_rep = sizes
    dist = []
    for r in range(n_row):
        if packed:
            rows = got[r].reshape(-1, got.shape[-1])
            value = jnp.dot(pick[...], rows, preferred_element_type=F32).astype(BF16)
        else:
            value = jnp.max(got[r], axis=0)
        dist.append(jnp.maximum(value, hot[r]))
    here = lax.axis_index("row")
    value = dist[0]
    for r in range(1, n_row):
        value = jnp.where(here == r, dist[r], value)
    own[...] = value
    relax(dist, edges, best)
    part[:, 0] = best[...].astype(BF16)
    relax(dist, theirs.at[pl.ds(n_row * n_col, n_row * n_col)], best)
    part[:, 1] = best[...].astype(BF16)


def merge_kernel(fresh, own, merged):
    merged[0] = jnp.maximum(jnp.max(fresh[:, 0], axis=0), own[...])
    merged[1] = jnp.max(fresh[:, 1], axis=0)


def decode(code):
    code = code.astype(F32)
    level = jnp.ceil((TOP - 0.22 - jnp.log2(jnp.maximum(code, 2.0**-125))) / STEP)
    value = jnp.where(code > 0.0, level, FAR)
    return jnp.where(value > 0.0, value, 0.0)


def final_kernel(mine, theirs, distances, sums):
    value = decode(jnp.maximum(mine[0], theirs[1]))
    other = decode(jnp.maximum(mine[1], theirs[0]))
    distances[...] = value
    inverse = jnp.where(value > 0.0, 1.0 / jnp.maximum(value, 1.0), 0.0)
    inverse += jnp.where(other > 0.0, 1.0 / jnp.maximum(other, 1.0), 0.0)
    sums[...] = jnp.sum(inverse.T, axis=0, keepdims=True)


def in_hbm(array):
    return pltpu.with_memory_space_constraint(array, pltpu.HBM)


def per_device(sources, tile_weights, tile_src, tile_dst, tile_count):
    sizes = n_row, n_col, n_rep = tuple(lax.axis_size(a) for a in ("row", "col", "rep"))
    height = sources.shape[0]
    tiles, size, _ = tile_weights.shape
    slots = n_row * n_rep
    room = min(height, max(16, 3 * height // (2 * n_col)))
    assert n_rep == 2 and all(n & (n - 1) == 0 for n in (*sizes, size))
    vmem = pl.BlockSpec(memory_space=pltpu.VMEM)
    smem = pl.BlockSpec(memory_space=pltpu.SMEM)
    hbm = pl.BlockSpec(memory_space=pltpu.HBM)
    limit = pltpu.CompilerParams(vmem_limit_bytes=28 << 20)
    shape = jax.ShapeDtypeStruct
    swap = [(i, (i + 1) % n_rep) for i in range(n_rep)]
    places = slots * n_col + 1
    best = pltpu.VMEM((n_col, height, size), F32)
    edges, hot, pick, part, over = pl.pallas_call(
        functools.partial(first_kernel, sizes),
        out_shape=(
            shape((places, size, size), BF16),
            shape((slots, height, size), BF16),
            shape((height, n_col * room), BF16),
            shape((n_row, n_col, room, size), BF16),
            pltpu.SMEM((1,), jnp.int32),
        ),
        in_specs=[hbm] * 4 + [smem],
        out_specs=(vmem,) * 4 + (smem,),
        scratch_shapes=[
            pltpu.VMEM((slots, room, size), BF16),
            pltpu.VMEM((n_col, room, size), F32),
            pltpu.VMEM((tiles, size, size), jnp.int32),
            pltpu.VMEM((1, height), jnp.int32),
            pltpu.SMEM((tiles,), jnp.int32),
            pltpu.SMEM((tiles,), jnp.int32),
            pltpu.SemaphoreType.DMA((CHUNKS,)),
            pltpu.SemaphoreType.DMA((3,)),
        ],
        compiler_params=limit,
        name="round_one",
    )(*map(in_hbm, (sources.reshape(1, height), tile_weights, tile_src, tile_dst)), tile_count)

    def finish(packed, part, hot, pick, edges):
        theirs = lax.ppermute(edges, "rep", swap)
        got = lax.all_to_all(
            part.reshape(n_row * n_col, *part.shape[2:]), ("row", "col"), 0, 0
        ).reshape(part.shape)
        return pl.pallas_call(
            functools.partial(second_kernel, sizes, packed),
            out_shape=(shape((n_col, n_rep, height, size), BF16), shape((height, size), BF16)),
            in_specs=[vmem] * 5,
            out_specs=(vmem,) * 2,
            scratch_shapes=[best],
            compiler_params=limit,
            name="round_two" if packed else "round_two_all",
        )(got, hot, pick, edges, theirs)

    def common(part, hot, pick, edges):
        return finish(True, part, hot, pick, edges)

    def crowded(part, hot, pick, edges):
        full = pl.pallas_call(
            first_kernel_all,
            out_shape=shape((n_row, n_col, height, size), BF16),
            in_specs=[vmem] * 2,
            out_specs=vmem,
            scratch_shapes=[best],
            compiler_params=limit,
            name="round_one_all",
        )(hot, edges)
        return finish(False, full, hot, pick, edges)

    part, own = lax.cond(over[0] > 0, crowded, common, part, hot, pick, edges)
    fresh = lax.all_to_all(part, "col", 0, 0)
    mine = pl.pallas_call(
        merge_kernel,
        out_shape=shape((n_rep, height, size), BF16),
        in_specs=[vmem] * 2,
        out_specs=vmem,
        compiler_params=limit,
        name="merge",
    )(fresh, own)
    theirs = lax.ppermute(mine, "rep", swap)
    return pl.pallas_call(
        final_kernel,
        out_shape=(shape((height, size), F32), shape((1, height), F32)),
        in_specs=[vmem] * 2,
        out_specs=(vmem,) * 2,
        compiler_params=limit,
        name="decode",
    )(mine, theirs)


def solution(mesh):
    cut = ("row", "col", "rep")
    return jax.shard_map(
        per_device,
        mesh=mesh,
        in_specs=(P(), P(cut, None, None), P(cut), P(cut), P(cut)),
        out_specs=(P(None, cut), P(("row", "col"), None)),
        check_vma=False,
    )
```

```python
import functools

import jax
import jax.numpy as jnp
from jax import lax
from jax.experimental import pallas as pl
from jax.experimental.pallas import tpu as pltpu
from jax.sharding import PartitionSpec as P

BLK_DEV = 1
STEP = 7.5
TOP = 126.0
FAR = 255.0
CHUNKS = 4
F32, BF16 = jnp.float32, jnp.bfloat16


def relax(dist, edges, best):
    width = best.shape[0]
    for q, left in enumerate(dist):
        for d in range(width):
            total = jnp.dot(left, edges[q * width + d], preferred_element_type=F32)
            best[d] = jnp.maximum(best[d], total) if q else total


def log(n):
    return n.bit_length() - 1


def column_of(vertex, size, n_col, n_rep):
    return lax.shift_right_logical(vertex, log(size * n_rep)) & (n_col - 1)


def spread(part, best):
    coded = best[...].astype(BF16)
    for r in range(part.shape[0]):
        part[r] = coded


def first_kernel(
    sizes, sources, weights, src, dst, count,
    edges, hot, pick, part, over,
    few, best, raw, ids, s_src, s_dst, sems, small,
):
    n_row, n_col, n_rep = sizes
    tiles, size, _ = raw.shape
    height, room = hot.shape[1], few.shape[1]
    step = tiles // CHUNKS
    firsts = [
        pltpu.make_async_copy(a, b, small.at[i])
        for i, (a, b) in enumerate(((sources, ids), (src, s_src), (dst, s_dst)))
    ]
    for copy in firsts:
        copy.start()
    copies = [
        pltpu.make_async_copy(
            weights.at[pl.ds(c * step, step)], raw.at[pl.ds(c * step, step)], sems.at[c]
        )
        for c in range(CHUNKS)
    ]
    live = count[0]
    for c, copy in enumerate(copies):
        pl.when(c * step < live)(copy.start)
    edges[...] = jnp.zeros_like(edges)
    for copy in firsts:
        copy.wait()
    me = lax.axis_index("col")
    along = jnp.broadcast_to(ids[...], (size, height))
    down = along.T
    lane = lax.broadcasted_iota(jnp.int32, (height, size), 1)
    col_along = column_of(along[:height], size, n_col, n_rep)
    col_down = column_of(down, size, n_col, n_rep)
    s_a = lax.broadcasted_iota(jnp.int32, (height, height), 1)
    s_d = lax.broadcasted_iota(jnp.int32, (height, height), 0)
    same = col_along == col_down[:, :height]
    rank_down = jnp.sum(jnp.where(same & (s_a < s_d), 1.0, 0.0), axis=1, keepdims=True)
    rank_along = jnp.sum(jnp.where(same & (s_d < s_a), 1.0, 0.0), axis=0, keepdims=True)
    over[0] = (jnp.max(rank_along) >= room).astype(jnp.int32)
    place = lax.broadcasted_iota(jnp.int32, (height, n_col * room), 1)
    slot = jnp.where(rank_down < room, rank_down + room * col_down[:, :1].astype(F32), -1.0)
    pick[...] = jnp.where(place.astype(F32) == slot, 1.0, 0.0).astype(BF16)
    order = lax.broadcasted_iota(jnp.int32, (room, height), 0).astype(F32)
    taken = (order == rank_along) & (col_along[:room] == me)
    vertex = jnp.sum(jnp.where(taken, along[:room].astype(F32) + 1.0, 0.0), axis=1, keepdims=True) - 1.0
    rep = lax.axis_index("rep")
    for q in range(n_row * n_rep):
        at = lane + ((q % n_row * n_col + me) * n_rep + (rep ^ (q // n_row))) * size
        hot[q] = jnp.where(down == at, 2.0**TOP, 0.0).astype(BF16)
        few[q] = jnp.where(vertex == at[:room].astype(F32), 2.0**TOP, 0.0).astype(BF16)
    for c, copy in enumerate(copies):

        @pl.when(c * step < live)
        def _(c=c, copy=copy):
            copy.wait()
            for k in range(c * step, (c + 1) * step):
                q = ((s_src[k] & 1) ^ rep) * n_row + lax.shift_right_logical(s_src[k], log(n_col * n_rep))
                d = lax.shift_right_logical(s_dst[k], log(n_rep)) & (n_col - 1)
                at = jnp.where(k < live, q * n_col + d, n_row * n_rep * n_col)
                w = raw[k].astype(F32).astype(BF16)
                coded = jnp.where(w > 0, jnp.exp2(BF16(-STEP) * w), BF16(0.0))
                edges[at] = jnp.maximum(edges[at], coded)

    relax([few[q] for q in range(n_row * n_rep)], edges, best)
    spread(part, best)


def first_kernel_all(hot, edges, part, best):
    relax([hot[q] for q in range(hot.shape[0])], edges, best)
    spread(part, best)


def second_kernel(sizes, packed, got, hot, pick, edges, theirs, part, own, best):
    n_row, n_col, n_rep = sizes
    dist = []
    for r in range(n_row):
        if packed:
            rows = got[r].reshape(-1, got.shape[-1])
            value = jnp.dot(pick[...], rows, preferred_element_type=F32).astype(BF16)
        else:
            value = jnp.max(got[r], axis=0)
        dist.append(jnp.maximum(value, hot[r]))
    here = lax.axis_index("row")
    value = dist[0]
    for r in range(1, n_row):
        value = jnp.where(here == r, dist[r], value)
    own[...] = value
    relax(dist, edges, best)
    part[:, 0] = best[...].astype(BF16)
    relax(dist, theirs.at[pl.ds(n_row * n_col, n_row * n_col)], best)
    part[:, 1] = best[...].astype(BF16)


def merge_kernel(fresh, own, merged):
    merged[0] = jnp.maximum(jnp.max(fresh[:, 0], axis=0), own[...])
    merged[1] = jnp.max(fresh[:, 1], axis=0)


def decode(code):
    code = code.astype(F32)
    level = jnp.ceil((TOP - 0.22 - jnp.log2(jnp.maximum(code, 2.0**-125))) / STEP)
    value = jnp.where(code > 0.0, level, FAR)
    return jnp.where(value > 0.0, value, 0.0)


def final_kernel(mine, theirs, distances, sums):
    value = decode(jnp.maximum(mine[0], theirs[1]))
    other = decode(jnp.maximum(mine[1], theirs[0]))
    distances[...] = value
    inverse = jnp.where(value > 0.0, 1.0 / jnp.maximum(value, 1.0), 0.0)
    inverse += jnp.where(other > 0.0, 1.0 / jnp.maximum(other, 1.0), 0.0)
    sums[...] = jnp.sum(inverse.T, axis=0, keepdims=True)


def in_hbm(array):
    return pltpu.with_memory_space_constraint(array, pltpu.HBM)


def per_device(sources, tile_weights, tile_src, tile_dst, tile_count):
    sizes = n_row, n_col, n_rep = tuple(lax.axis_size(a) for a in ("row", "col", "rep"))
    height = sources.shape[0]
    tiles, size, _ = tile_weights.shape
    slots = n_row * n_rep
    room = min(height, max(16, 3 * height // (2 * n_col)))
    assert n_rep == 2 and all(n & (n - 1) == 0 for n in (*sizes, size))
    vmem = pl.BlockSpec(memory_space=pltpu.VMEM)
    smem = pl.BlockSpec(memory_space=pltpu.SMEM)
    hbm = pl.BlockSpec(memory_space=pltpu.HBM)
    limit = pltpu.CompilerParams(vmem_limit_bytes=28 << 20)
    shape = jax.ShapeDtypeStruct
    swap = [(i, (i + 1) % n_rep) for i in range(n_rep)]
    places = slots * n_col + 1
    best = pltpu.VMEM((n_col, height, size), F32)
    edges, hot, pick, part, over = pl.pallas_call(
        functools.partial(first_kernel, sizes),
        out_shape=(
            shape((places, size, size), BF16),
            shape((slots, height, size), BF16),
            shape((height, n_col * room), BF16),
            shape((n_row, n_col, room, size), BF16),
            pltpu.SMEM((1,), jnp.int32),
        ),
        in_specs=[hbm] * 4 + [smem],
        out_specs=(vmem,) * 4 + (smem,),
        scratch_shapes=[
            pltpu.VMEM((slots, room, size), BF16),
            pltpu.VMEM((n_col, room, size), F32),
            pltpu.VMEM((tiles, size, size), jnp.int32),
            pltpu.VMEM((1, height), jnp.int32),
            pltpu.SMEM((tiles,), jnp.int32),
            pltpu.SMEM((tiles,), jnp.int32),
            pltpu.SemaphoreType.DMA((CHUNKS,)),
            pltpu.SemaphoreType.DMA((3,)),
        ],
        compiler_params=limit,
        name="round_one",
    )(*map(in_hbm, (sources.reshape(1, height), tile_weights, tile_src, tile_dst)), tile_count)

    def finish(packed, part, hot, pick, edges):
        theirs = lax.ppermute(edges, "rep", swap)
        got = lax.all_to_all(
            part.reshape(n_row * n_col, *part.shape[2:]), ("row", "col"), 0, 0
        ).reshape(part.shape)
        return pl.pallas_call(
            functools.partial(second_kernel, sizes, packed),
            out_shape=(shape((n_col, n_rep, height, size), BF16), shape((height, size), BF16)),
            in_specs=[vmem] * 5,
            out_specs=(vmem,) * 2,
            scratch_shapes=[best],
            compiler_params=limit,
            name="round_two" if packed else "round_two_all",
        )(got, hot, pick, edges, theirs)

    def common(part, hot, pick, edges):
        return finish(True, part, hot, pick, edges)

    def crowded(part, hot, pick, edges):
        full = pl.pallas_call(
            first_kernel_all,
            out_shape=shape((n_row, n_col, height, size), BF16),
            in_specs=[vmem] * 2,
            out_specs=vmem,
            scratch_shapes=[best],
            compiler_params=limit,
            name="round_one_all",
        )(hot, edges)
        return finish(False, full, hot, pick, edges)

    part, own = lax.cond(over[0] > 0, crowded, common, part, hot, pick, edges)
    fresh = lax.all_to_all(part, "col", 0, 0)
    mine = pl.pallas_call(
        merge_kernel,
        out_shape=shape((n_rep, height, size), BF16),
        in_specs=[vmem] * 2,
        out_specs=vmem,
        compiler_params=limit,
        name="merge",
    )(fresh, own)
    theirs = lax.ppermute(mine, "rep", swap)
    return pl.pallas_call(
        final_kernel,
        out_shape=(shape((height, size), F32), shape((1, height), F32)),
        in_specs=[vmem] * 2,
        out_specs=(vmem,) * 2,
        compiler_params=limit,
        name="decode",
    )(mine, theirs)


def solution(mesh):
    cut = ("row", "col", "rep")
    return jax.shard_map(
        per_device,
        mesh=mesh,
        in_specs=(P(), P(cut, None, None), P(cut), P(cut), P(cut)),
        out_specs=(P(None, cut), P(("row", "col"), None)),
        check_vma=False,
    )
```
